32 devices in a mesh: dom: 32 (over z, y, x, core).
Axes of the slice: x: 2, y: 2, z: 4, core: 2. Of those that a mesh axis runs over, the one named last changes fastest.
Arguments:
- right_side: float32 [32768, 3], P('dom'), may hold values from -10 to 10
- fine_diagonal: float32 [32768, 3], P('dom'), may hold values from 2 to 4
- fine_columns: int32 [32768, 27], P('dom'), may hold values from 0 to 32767, as said below
- fine_blocks: float32 [32768, 27, 3, 3], P('dom'), may hold values from -0.625 to 0.625
- aggregate_of_node: int32 [32768], P('dom'), may hold values from 0 to 31, as said below
- coarse_row_of_aggregate: int32 [1024], P('dom'), may hold values from 0 to 1023, as said below
- coarse_diagonal: float32 [1024, 3], P('dom'), may hold values from 2 to 4
- coarse_columns: int32 [1024, 27], P('dom'), may hold values from 0 to 1023
- coarse_blocks: float32 [1024, 27, 3, 3], P('dom'), may hold values from -0.625 to 0.625
Outputs:
- solution: float32 [32768, 3], P('dom')
- correction: float32 [1024, 3], P('dom')
The draws below stay inside these ranges and needn't reach their ends.
Inputs may be any that keep to these rules, and one draw needn't show every extreme that they name: Every entry of fine_columns differs from its row number by at most 256, and some entry by exactly 256. `aggregate_of_node`: on each device every aggregate number 0 to 31 is used by at least one of its nodes. coarse_row_of_aggregate is a permutation of 0 to 1023; among the 32 aggregates of one device (an aligned block of entries) at most 8 get rows of any one owner, and exactly 8 for some owner.
All inputs are finite; a program needn't handle non-finite values.
Results may differ from the reference program's by a relative error of at most 0.0003.
Values sent between devices are 32-bit elements.
A program may use at most 64 MiB of HBM per device.

```python
import jax
import jax.numpy as jnp
from jax import lax

NODE_DEV = 1024
CAP = 8
WIN = 256
NNZ = 27
CNNZ = 27
SWEEPS = 2
CSWEEPS = 6
AGG_DEV = 32
NODES = 32768
AGGS = 1024


def draw_fine_columns(key, part):
    row_ids = jnp.arange(NODES, dtype=jnp.int32)[:, None]
    offset = jax.random.randint(jax.random.fold_in(key, 13), (NODES, NNZ), -WIN, WIN + 1)
    columns = jnp.clip(row_ids + offset, 0, NODES - 1)
    return columns.at[0, 0].set(WIN).astype(jnp.int32)


def draw_aggregate_of_node(key, part):
    devices = NODES // NODE_DEV
    key_raw, key_mix = jax.random.split(jax.random.fold_in(key, 11))
    labels_raw = jax.random.randint(key_raw, (devices, NODE_DEV), 0, AGG_DEV)
    labels_raw = labels_raw.at[:, :AGG_DEV].set(jnp.arange(AGG_DEV, dtype=jnp.int32)[None, :])
    mixers = jax.random.split(key_mix, devices)
    shuffles = jax.vmap(lambda one_key: jax.random.permutation(one_key, NODE_DEV))(mixers)
    return jnp.take_along_axis(labels_raw, shuffles, axis=1).reshape(-1).astype(jnp.int32)


def draw_coarse_row_of_aggregate(key, part):
    devices = AGGS // AGG_DEV
    groups = AGG_DEV // CAP
    key_group, key_slot, key_label = jax.random.split(jax.random.fold_in(key, 17), 3)
    scores = jax.random.permutation(key_group, devices).astype(jnp.int32)
    scores = scores.at[devices // 2].set(-3).at[1].set(-2).at[devices - 1].set(-1)
    offsets = jnp.argsort(scores, stable=True)[:groups].astype(jnp.int32)
    sources = jnp.arange(devices, dtype=jnp.int32)[:, None]
    label_mix = jax.vmap(lambda one_key: jax.random.permutation(one_key, AGG_DEV))(jax.random.split(key_label, devices)).astype(jnp.int32)
    group_ids = label_mix // CAP
    owners = (sources + offsets[group_ids]) % devices
    within = group_ids * CAP + label_mix % CAP
    slot_mix = jax.vmap(lambda one_key: jax.random.permutation(one_key, AGG_DEV))(jax.random.split(key_slot, devices)).astype(jnp.int32)
    slots = slot_mix[owners, within]
    return (owners * AGG_DEV + slots).reshape(-1).astype(jnp.int32)


def with_ends(drawn, own_key, low, high):
    spot = [jax.random.randint(jax.random.fold_in(own_key, axis), (), 0, length) for axis, length in enumerate(drawn.shape)]
    main_axis = drawn.shape.index(max(drawn.shape))
    neighbour = spot[:main_axis] + [(spot[main_axis] + 1) % drawn.shape[main_axis]] + spot[main_axis + 1:]
    return drawn.at[tuple(spot)].set(low).at[tuple(neighbour)].set(high)


def level_of(own_key, extent, cuts, low, high):
    loudness, own = 1.0, jax.random.fold_in(own_key, 6)
    for dim, blocks in cuts:
        draws = jnp.exp(jax.random.uniform(jax.random.fold_in(own, dim), (blocks,), jnp.float32, low / len(cuts), high / len(cuts)))
        loudness = loudness * jnp.repeat(draws, extent[dim] // blocks).reshape([-1 if axis == dim else 1 for axis in range(len(extent))])
    return loudness


def bell_draw(key, shape, scale, reach, cuts=(), kind=jnp.bfloat16):
    gain = level_of(key, shape, cuts, -0.22, 0.18) if cuts else 1.0
    values = jax.random.normal(key, shape, jnp.float32) * scale * gain
    return jnp.minimum(jnp.maximum(values, -reach), reach).astype(kind)


def setup_inputs(seed: int = 0) -> dict:
    seeds = jax.random.split(jax.random.key(seed), 10)
    return {
        "right_side": bell_draw(seeds[0], (NODES, 3), 2.0, 10.0, ((0, 32),), jnp.float32),
        "fine_diagonal": jnp.clip(2.0 + 2.0 * jax.random.uniform(seeds[1], (NODES, 3), jnp.float32) ** level_of(seeds[1], (NODES, 3), ((0, 32),), -0.2, 0.2), 2.0, 4.0),
        "fine_columns": draw_fine_columns(jax.random.fold_in(seeds[9], 71), 0),
        "fine_blocks": bell_draw(seeds[3], (NODES, NNZ, 3, 3), (3 * NNZ) ** -0.5, 0.625, ((0, 32),), jnp.float32),
        "aggregate_of_node": draw_aggregate_of_node(jax.random.fold_in(seeds[9], 71), 0),
        "coarse_row_of_aggregate": draw_coarse_row_of_aggregate(jax.random.fold_in(seeds[9], 71), 0),
        "coarse_diagonal": jnp.clip(2.0 + 2.0 * jax.random.uniform(seeds[6], (AGGS, 3), jnp.float32) ** level_of(seeds[6], (AGGS, 3), ((0, 32),), -0.2, 0.2), 2.0, 4.0),
        "coarse_columns": with_ends(jax.random.randint(seeds[7], (AGGS, CNNZ), 0, AGGS), jax.random.fold_in(seeds[7], 1), 0, AGGS - 1).astype(jnp.int32),
        "coarse_blocks": bell_draw(seeds[8], (AGGS, CNNZ, 3, 3), (3 * CNNZ) ** -0.5, 0.625, ((0, 32),), jnp.float32),
    }


damping = 0.7


def apply_level(field, diagonal, columns, blocks):
    nearby = field[columns]
    pulled = jnp.einsum("rkij,rkj->ri", blocks, nearby, precision=lax.Precision.HIGHEST)
    return diagonal * field - pulled


def reference(right_side, fine_diagonal, fine_columns, fine_blocks, aggregate_of_node, coarse_row_of_aggregate, coarse_diagonal, coarse_columns, coarse_blocks):
    solution = jnp.zeros_like(right_side)
    for sweep in range(SWEEPS):
        solution = solution + damping * (right_side - apply_level(solution, fine_diagonal, fine_columns, fine_blocks)) / fine_diagonal
    residual = right_side - apply_level(solution, fine_diagonal, fine_columns, fine_blocks)
    node_ids = jnp.arange(NODES, dtype=jnp.int32)
    labels = (node_ids // NODE_DEV) * AGG_DEV + aggregate_of_node
    coarse_rows = coarse_row_of_aggregate[labels]
    coarse_rhs = jax.ops.segment_sum(residual, coarse_rows, num_segments=AGGS)
    correction = jnp.zeros_like(coarse_rhs)
    for sweep in range(CSWEEPS):
        correction = correction + damping * (coarse_rhs - apply_level(correction, coarse_diagonal, coarse_columns, coarse_blocks)) / coarse_diagonal
    solution = solution + correction[coarse_rows]
    for sweep in range(SWEEPS):
        solution = solution + damping * (right_side - apply_level(solution, fine_diagonal, fine_columns, fine_blocks)) / fine_diagonal
    return solution, correction
```

```python
import functools

import jax
import jax.numpy as jnp
from jax import lax
from jax.experimental import pallas as pl
from jax.experimental.pallas import tpu as pltpu
from jax.sharding import PartitionSpec as P

WIN = 256
SWEEPS = 2
CSWEEPS = 6
LANES = 128

damping = 0.7


def pick(source, lane):
    return jnp.take_along_axis(source, lane, axis=1, mode="promise_in_bounds")


def fine_kernel(smooth, pad_ref, index_ref, block_ref, diagonal_ref, right_ref, out_ref):
    slots, chunks, _ = index_ref.shape
    margin = WIN // LANES
    sources = [[pad_ref[c, j : j + chunks, :] for j in range(2 * margin + 1)] for c in range(3)]
    total = [jnp.zeros((chunks, LANES), jnp.float32) for _ in range(3)]
    for k in range(slots):
        position = index_ref[k]
        lane, chunk = position & (LANES - 1), position >> 7
        masks = [chunk == j for j in range(2 * margin + 1)]
        for c in range(3):
            near = pick(sources[c][0], lane)
            for j in range(1, 2 * margin + 1):
                near = jnp.where(masks[j], pick(sources[c][j], lane), near)
            for i in range(3):
                total[i] = total[i] + block_ref[k, i, c] * near
    for i in range(3):
        field = pad_ref[i, margin : margin + chunks, :]
        residual = right_ref[i] - (diagonal_ref[i] * field - total[i])
        if smooth:
            out_ref[i] = field + damping * residual / diagonal_ref[i]
        else:
            out_ref[i] = residual


def far_pick(values, position):
    lane, chunk = position & (LANES - 1), position >> 7
    out = []
    for value in values:
        count = value.shape[0]
        near = jnp.zeros(position.shape, jnp.float32)
        for j in range(count):
            row = jnp.broadcast_to(value[j : j + 1, :], position.shape)
            near = jnp.where(chunk == j, pick(row, lane), near)
        out.append(near)
    return out


def coarse_kernel(sums_ref, inverse_ref, column_ref, block_ref, diagonal_ref, label_ref, own_ref, field_ref,
                  out_ref, correction_ref, rhs_ref, next_ref):
    slots, chunks, _ = column_ref.shape
    group = 8
    groups = chunks // group
    for g in range(groups):
        rows = pl.ds(g * group, group)
        picked = far_pick([sums_ref[c] for c in range(3)], inverse_ref[rows, :])
        for c in range(3):
            rhs_ref[c, rows, :] = picked[c]
            correction_ref[c, rows, :] = damping * picked[c] / diagonal_ref[c, rows, :]

    def sweep(_, carry):
        for g in range(groups):
            rows = pl.ds(g * group, group)

            def slot(k, total):
                total = list(total)
                near = far_pick([correction_ref[c] for c in range(3)], column_ref[k, rows, :])
                for i in range(3):
                    for c in range(3):
                        total[i] = total[i] + block_ref[k, i, c, rows, :] * near[c]
                return tuple(total)

            zero = jnp.zeros((group, LANES), jnp.float32)
            total = lax.fori_loop(0, slots, slot, (zero,) * 3, unroll=9 if groups == 1 else 1)
            for i in range(3):
                diagonal, field = diagonal_ref[i, rows, :], correction_ref[i, rows, :]
                residual = rhs_ref[i, rows, :] - (diagonal * field - total[i])
                next_ref[i, rows, :] = field + damping * residual / diagonal
        correction_ref[...] = next_ref[...]
        return carry

    lax.fori_loop(0, CSWEEPS - 1, sweep, 0)
    label = label_ref[...]
    row = pick(jnp.broadcast_to(own_ref[...], label.shape), label)
    picked = far_pick([correction_ref[c] for c in range(3)], row)
    for c in range(3):
        out_ref[c] = field_ref[c] + picked[c]


def per_device(
    right_side,
    fine_diagonal,
    fine_columns,
    fine_blocks,
    aggregate_of_node,
    coarse_row_of_aggregate,
    coarse_diagonal,
    coarse_columns,
    coarse_blocks,
):
    devices, me = lax.axis_size("dom"), lax.axis_index("dom")
    nodes, slots = fine_columns.shape
    chunks, margin = nodes // LANES, WIN // LANES
    own, coarse_slots = coarse_columns.shape
    rows = own * devices
    up = [(i, i + 1) for i in range(devices - 1)]
    down = [(j, i) for i, j in up]

    right = right_side.T.reshape(3, chunks, LANES)
    diagonal = fine_diagonal.T.reshape(3, chunks, LANES)
    blocks = jnp.transpose(fine_blocks, (1, 2, 3, 0)).reshape(slots, 3, 3, chunks, LANES)
    shift = LANES * jnp.arange(chunks, dtype=jnp.int32)[None, :, None]
    index = fine_columns.T.reshape(slots, chunks, LANES) - (me * nodes - WIN) - shift
    label = aggregate_of_node.reshape(chunks, LANES)

    floats = jnp.concatenate(
        [jnp.transpose(coarse_blocks, (1, 2, 3, 0)).reshape(coarse_slots * 9, own), coarse_diagonal.T], axis=0
    )
    integers = jnp.concatenate([coarse_columns.T, coarse_row_of_aggregate[None, :]], axis=0)
    floats = lax.all_gather(floats, "dom", axis=1, tiled=True)
    integers = lax.all_gather(integers, "dom", axis=1, tiled=True)
    grid = (rows // LANES, LANES)
    all_blocks = floats[: coarse_slots * 9].reshape((coarse_slots, 3, 3) + grid)
    all_diagonal = floats[coarse_slots * 9 :].reshape((3,) + grid)
    all_columns = integers[:coarse_slots].reshape((coarse_slots,) + grid)
    permutation = integers[coarse_slots]
    ids = jnp.arange(rows, dtype=jnp.int32)
    inverse = jnp.sum(jnp.where(permutation[:, None] == ids[None, :], ids[:, None], 0), axis=0).reshape(grid)
    own_rows = jnp.pad(coarse_row_of_aggregate, (0, LANES - own)).reshape(1, LANES)

    def fine(field, smooth):
        before = lax.ppermute(field[:, chunks - margin :], "dom", up)
        after = lax.ppermute(field[:, :margin], "dom", down)
        padded = jnp.concatenate([before, field, after], axis=1)
        return pl.pallas_call(
            functools.partial(fine_kernel, smooth),
            out_shape=jax.ShapeDtypeStruct((3, chunks, LANES), jnp.float32),
        )(padded, index, blocks, diagonal, right)

    field = damping * right / diagonal
    for _ in range(SWEEPS - 1):
        field = fine(field, True)
    residual = fine(field, False)
    member = aggregate_of_node[None, :] == jnp.arange(own, dtype=jnp.int32)[:, None]
    flat = residual.reshape(3, nodes)
    sums = jnp.sum(jnp.where(member[None], flat[:, None, :], 0.0), axis=2)
    sums = lax.all_gather(sums, "dom", axis=1, tiled=True).reshape((3,) + grid)
    field, correction = pl.pallas_call(
        coarse_kernel,
        out_shape=(
            jax.ShapeDtypeStruct((3, chunks, LANES), jnp.float32),
            jax.ShapeDtypeStruct((3,) + grid, jnp.float32),
        ),
        scratch_shapes=[pltpu.VMEM((3,) + grid, jnp.float32), pltpu.VMEM((3,) + grid, jnp.float32)],
    )(sums, inverse, all_columns, all_blocks, all_diagonal, label, own_rows, field)
    correction = lax.dynamic_slice_in_dim(correction.reshape(3, rows), me * own, own, axis=1).T
    for _ in range(SWEEPS):
        field = fine(field, True)
    return (field.reshape(3, nodes).T, correction)


def solution(mesh):
    return jax.shard_map(
        per_device,
        mesh=mesh,
        in_specs=(
            P("dom", None),
            P("dom", None),
            P("dom", None),
            P("dom", None, None, None),
            P("dom"),
            P("dom"),
            P("dom", None),
            P("dom", None),
            P("dom", None, None, None),
        ),
        out_specs=(P("dom", None), P("dom", None)),
        check_vma=False,
    )
```
